32 devices in a mesh: kv: 16 (over z, x, core), tp: 2 (over y).
Axes of the slice: x: 2, y: 2, z: 4, core: 2. Of those that a mesh axis runs over, the one named last changes fastest.
Arguments:
- queries: bfloat16 [16, 128, 576], P(None, 'tp'), may hold values from -36 to 36
- cache: bfloat16 [16, 4096, 576], P(None, 'kv'), may hold values from -6 to 6
- lengths: int32 [16], replicated, may hold values from 1 to 4096, as said below
- w_ov: bfloat16 [128, 512, 7168], P('tp', None, 'kv'), may hold values from -0.0234375 to 0.0234375
- resid: bfloat16 [16, 7168], P(None, 'tp'), may hold values from -3 to 3
- gain: float32 [7168], P('tp'), may hold values from 0.5 to 1.5
- w_gate: bfloat16 [7168, 18432], P('tp', 'kv'), may hold values from -0.0625 to 0.0625
- w_up: bfloat16 [7168, 18432], P('tp', 'kv'), may hold values from -0.0625 to 0.0625
- w_down: bfloat16 [18432, 7168], P('kv', 'tp'), may hold values from -0.046875 to 0.046875
Outputs:
- layer_out: bfloat16 [16, 7168], P(None, 'tp')
The draws below stay inside these ranges and needn't reach their ends.
Inputs may be any that keep to these rules, and one draw needn't show every extreme that they name: Sequence b attends to positions 0 to lengths[b] - 1; in every draw some sequence has all 4096 positions live.
All inputs are finite; a program needn't handle non-finite values.
Results may differ from the reference program's by a relative error of at most 0.006.
Values sent between devices are 32-bit elements; how exact they have to be, the bound alone decides.
A program may use at most 128 MiB of HBM per device.

```python
import jax
import jax.numpy as jnp
from jax import lax

D = 7168
HEADS = 128
LAT = 512
ROPE = 64
FF = 18432
BATCH = 16
CTX_DEV = 256
CTX = 4096
N_KV = 16


def cache_values(key):
    raw = jax.random.normal(jax.random.fold_in(key, 11), (BATCH, CTX, LAT + ROPE), jnp.float32)
    return jnp.clip(raw, -6.0, 6.0)


def draw_cache(key, part):
    return cache_values(key).astype(jnp.bfloat16)


def draw_queries(key, part):
    base = jax.random.normal(jax.random.fold_in(key, 12), (BATCH, HEADS, LAT + ROPE), jnp.float32)
    base = jnp.clip(base, -6.0, 6.0)
    return base.astype(jnp.bfloat16)


def draw_lengths(key, part):
    spans = jax.random.randint(jax.random.fold_in(key, 14), (BATCH,), 1, CTX + 1)
    longest = jax.random.randint(jax.random.fold_in(key, 15), (), 0, BATCH)
    return jnp.where(jnp.arange(BATCH, dtype=jnp.int32) == longest, CTX, spans).astype(jnp.int32)


def shard_levels(rng, shape, pieces, low, largest):
    def one(dim, blocks):
        heights = jax.random.uniform(jax.random.fold_in(jax.random.fold_in(rng, 6), dim), (blocks,), jnp.float32, low / len(pieces), largest / len(pieces))
        return jnp.repeat(jnp.exp(heights), shape[dim] // blocks).reshape((-1,) + (1,) * (len(shape) - dim - 1))

    loudness = one(*pieces[0])
    for cut in pieces[1:]:
        loudness = loudness * one(*cut)
    return loudness


def scatter_about(key, shape, spread, limit, shards=(), held_as=jnp.bfloat16):
    array = spread * jax.random.normal(key, shape, jnp.float32)
    if shards:
        array = array * shard_levels(key, shape, shards, -0.22, 0.18)
    return jnp.clip(array, -limit, limit).astype(held_as)


def setup_inputs(seed: int = 0) -> dict:
    key_of = jax.random.split(jax.random.key(seed), 10)
    return {
        "queries": draw_queries(jax.random.fold_in(key_of[9], 71), 0),
        "cache": draw_cache(jax.random.fold_in(key_of[9], 71), 0),
        "lengths": draw_lengths(jax.random.fold_in(key_of[9], 71), 0),
        "w_ov": scatter_about(key_of[3], (HEADS, LAT, D), (HEADS * LAT) ** -0.5, 0.0234375, ((0, 2), (2, 16))),
        "resid": scatter_about(key_of[4], (BATCH, D), 0.5, 3.0, ((1, 2),)),
        "gain": jnp.clip(1.0 + 0.1 * jax.random.normal(key_of[5], (D,), jnp.float32), 0.5, 1.5),
        "w_gate": scatter_about(key_of[6], (D, FF), D ** -0.5, 0.0625, ((0, 2), (1, 16))),
        "w_up": scatter_about(key_of[7], (D, FF), D ** -0.5, 0.0625, ((0, 2), (1, 16))),
        "w_down": scatter_about(key_of[8], (FF, D), FF ** -0.5, 0.046875, ((0, 16), (1, 2))),
    }


softmax_scale = 192.0 ** (-0.5)
masked_score = -1e+30
norm_floor = 0.05

def one_sequence(args):
    query, keys, length = args
    scores = jnp.dot(query, keys.T, preferred_element_type=jnp.float32) * softmax_scale
    place = jnp.arange(CTX, dtype=jnp.int32)
    live = place[None, :] < length
    scores = jnp.where(live, scores, masked_score).reshape(HEADS, N_KV, CTX_DEV)
    live = live.reshape(1, N_KV, CTX_DEV)
    peak = lax.optimization_barrier(jnp.max(scores, axis=2))
    weights = jnp.where(live, jnp.exp(scores - peak[:, :, None]), 0.0)
    total = lax.optimization_barrier(jnp.sum(weights, axis=2))
    rounded = lax.optimization_barrier(weights.astype(jnp.bfloat16))
    latent = keys[:, :LAT].astype(jnp.float32).reshape(N_KV, CTX_DEV, LAT)
    mixed = jnp.einsum('hnr,nrc->hnc', rounded.astype(jnp.float32), latent)
    top = lax.optimization_barrier(jnp.max(peak, axis=1))
    factor = jnp.exp(peak - top[:, None])
    whole = lax.optimization_barrier(jnp.sum(total * factor, axis=1))
    combined = lax.optimization_barrier(jnp.sum(mixed * factor[:, :, None], axis=1)) / whole[:, None]
    return combined.astype(jnp.bfloat16)

def reference(queries, cache, lengths, w_ov, resid, gain, w_gate, w_up, w_down):
    heads_out = lax.map(one_sequence, (queries, cache, lengths))
    attn = jnp.dot(heads_out.reshape(BATCH, HEADS * LAT), w_ov.reshape(HEADS * LAT, D), preferred_element_type=jnp.float32)
    state = resid.astype(jnp.float32) + attn
    meansq = lax.optimization_barrier(jnp.sum(state * state, axis=1)) / D
    scaled = (state * lax.rsqrt(meansq + norm_floor)[:, None] * gain[None, :]).astype(jnp.bfloat16)
    gate = jnp.dot(scaled, w_gate, preferred_element_type=jnp.float32)
    up = jnp.dot(scaled, w_up, preferred_element_type=jnp.float32)
    inner = (jax.nn.silu(gate) * up).astype(jnp.bfloat16)
    ffn = jnp.dot(inner, w_down, preferred_element_type=jnp.float32)
    return (state + ffn).astype(jnp.bfloat16)
```

```python
import functools

import jax
import jax.numpy as jnp
from jax import lax
from jax.experimental import pallas as pl
from jax.experimental.pallas import tpu as pltpu
from jax.sharding import PartitionSpec as P

LAT = 512
MESH = pl.DeviceIdType.MESH
F32 = jnp.float32
BF16 = jnp.bfloat16

softmax_scale = 192.0 ** (-0.5)
masked_score = -1e30
norm_floor = 0.05


def layer_kernel(
    n, nt, chunks, width_all,
    stats, mixed, resid, gain, wov_hbm, wg_hbm, wu_hbm, wd_hbm,
    out,
    sx, buf, r1, r2, r3, fin, wov, wg, wu, wd, pa, pr, pb, gath, st, sg, gu, gur, sqb, sqr,
    fp, f1, fa, f2, fb, f3, fin2,
    wsem, sx_s, sx_r, c_s, c_r, z_s, z_r, t_s, t_r, b_s, b_r, f_s, f_r, fz_s, fz_r,
):
    heads, batch, lat = mixed.shape
    nz = n // 4
    hc = heads // chunks
    half, quarter = hc // 2, hc // 4
    rows = quarter * batch // nz
    slots = wov.shape[0]
    me, tp = lax.axis_index("kv"), lax.axis_index("tp")
    c, x, z = lax.rem(me, 2), lax.rem(me // 2, 2), me // 4
    core_peer, x_peer = me + 1 - 2 * c, me + 2 - 4 * x

    def z_peer(d):
        return lax.rem(z + d, nz) * 4 + x * 2 + c

    def send(src, dst, s, r, **where):
        copy = pltpu.make_async_remote_copy(
            src_ref=src, dst_ref=dst, send_sem=s, recv_sem=r, device_id=where, device_id_type=MESH
        )
        copy.start()
        return copy

    loads = {}

    def load_ov(ch):
        loads[ch] = pltpu.make_async_copy(
            wov_hbm.at[pl.ds(ch * hc, hc)], wov.at[ch % slots], wsem.at[ch]
        )
        loads[ch].start()

    for ch in range(slots):
        load_ov(ch)
    others = []
    for i, (a, b) in enumerate(((wg_hbm, wg), (wu_hbm, wu), (wd_hbm, wd))):
        copy = pltpu.make_async_copy(a, b, wsem.at[chunks + i])
        copy.start()
        others.append(copy)

    barrier = pltpu.get_barrier_semaphore()
    for d in range(1, n):
        pl.semaphore_signal(barrier, inc=1, device_id={"kv": lax.rem(me + d, n)}, device_id_type=MESH)
    for d in range(1, nt):
        pl.semaphore_signal(barrier, inc=1, device_id={"tp": lax.rem(tp + d, nt)}, device_id_type=MESH)
    pl.semaphore_wait(barrier, n - 1 + nt - 1)

    copies = [
        send(stats, sx.at[d - 1], sx_s.at[d - 1], sx_r.at[d - 1], kv=lax.rem(me + d, n))
        for d in range(1, n)
    ]
    for copy in copies:
        copy.wait()
    peak, total = stats[0], stats[1]
    top = peak
    for d in range(n - 1):
        top = jnp.maximum(top, sx[d, 0])
    factor = jnp.exp(peak - top)
    whole = total * factor
    for d in range(n - 1):
        whole = whole + sx[d, 1] * jnp.exp(sx[d, 0] - top)
    factor = factor / whole

    def piece(ref, h0, zz):
        if rows % batch == 0:
            return ref.at[pl.ds(h0 + zz * (rows // batch), rows // batch)]
        return ref.at[h0 + zz * rows // batch, pl.ds(pl.multiple_of(lax.rem(zz * rows, batch), rows), rows)]

    flight = {}
    acc = [jnp.zeros((batch, pa.shape[1]), F32)]

    def stage(ch, s):
        b = ch * hc
        h0 = b + c * half
        q0 = h0 + x * quarter
        for copy in flight.pop(ch, ()):
            copy.wait()
        if s == 0:
            for i in range(hc):
                buf[b + i] = mixed[b + i] * factor[:, b + i : b + i + 1]
            flight[ch] = [
                send(buf.at[pl.ds(b + (1 - c) * half, half)], r1.at[ch], c_s.at[ch, 0], c_r.at[ch, 0], kv=core_peer)
            ]
        elif s == 1:
            for i in range(half):
                buf[h0 + i] = buf[h0 + i] + r1[ch, i]
            flight[ch] = [
                send(buf.at[pl.ds(h0 + (1 - x) * quarter, quarter)], r2.at[ch], c_s.at[ch, 1], c_r.at[ch, 1], kv=x_peer)
            ]
        elif s == 2:
            for i in range(quarter):
                buf[q0 + i] = buf[q0 + i] + r2[ch, i]
            flight[ch] = [
                send(piece(buf, q0, lax.rem(z + d, nz)), r3.at[ch, d - 1], z_s.at[ch, 0, d - 1], z_r.at[ch, 0, d - 1], kv=z_peer(d))
                for d in range(1, nz)
            ]
        elif s == 3:
            own = piece(buf, q0, z)[...]
            for d in range(nz - 1):
                own = own + r3[ch, d].reshape(own.shape)
            mine = piece(fin, q0, z)
            mine[...] = own
            flight[ch] = [
                send(mine, mine, z_s.at[ch, 1, d - 1], z_r.at[ch, 1, d - 1], kv=z_peer(d)) for d in range(1, nz)
            ]
        elif s == 4:
            part = fin.at[pl.ds(q0, quarter)]
            flight[ch] = [send(part, part, c_s.at[ch, 2], c_r.at[ch, 2], kv=x_peer)]
        elif s == 5:
            part = fin.at[pl.ds(h0, half)]
            flight[ch] = [send(part, part, c_s.at[ch, 3], c_r.at[ch, 3], kv=core_peer)]
        else:
            loads[ch].wait()

            def body(i, a):
                return a + jnp.dot(fin[b + i].astype(BF16), wov[ch % slots, i], preferred_element_type=F32)

            acc[0] = lax.fori_loop(0, hc, body, acc[0])
            if ch + slots < chunks:
                load_ov(ch + slots)

    for t in range(chunks + 6):
        turn = [(ch, t - ch) for ch in range(chunks) if 0 <= t - ch <= 6]
        for ch, s in sorted(turn, key=lambda e: e[1] == 6):
            stage(ch, s)

    pa[...] = acc[0]
    copies = [
        send(pa, pr.at[d - 1], t_s.at[0, d - 1], t_r.at[0, d - 1], tp=lax.rem(tp + d, nt)) for d in range(1, nt)
    ]
    own = pa[...]
    for copy in copies:
        copy.wait()
    for d in range(nt - 1):
        own = own + pr[d]
    pb[...] = own
    per = n // nt
    slot = lax.rem(me, per)
    owner = me // per == tp

    def spread(d):
        return pltpu.make_async_remote_copy(
            src_ref=pb, dst_ref=gath.at[slot], send_sem=b_s.at[d - 1], recv_sem=b_r.at[slot],
            device_id={"kv": lax.rem(me + d, n)}, device_id_type=MESH,
        )

    @pl.when(owner)
    def _():
        for d in range(1, n):
            spread(d).start()
        gath[slot] = pb[...]
        for d in range(1, n):
            spread(d).wait_send()

    for j in range(per):
        @pl.when(tp * per + j != me)
        def _():
            pltpu.make_async_remote_copy(
                src_ref=pb, dst_ref=gath.at[j], send_sem=b_s.at[0], recv_sem=b_r.at[j],
                device_id={"kv": me}, device_id_type=MESH,
            ).wait_recv()

    cols = pb.shape[1]
    for j in range(per):
        st[:, j * cols : (j + 1) * cols] = gath[j]
    state = st[...] + resid[...].astype(F32)
    st[...] = state
    sqb[...] = jnp.broadcast_to(jnp.sum(state * state, axis=1, keepdims=True), sqb.shape)
    sg[...] = (state * gain[...]).astype(BF16)

    width, hidden = wg.shape
    step = 512 if width % 512 == 0 else 128
    others[0].wait()
    others[1].wait()

    def project(i, carry):
        ga, ua = carry
        k = pl.ds(pl.multiple_of(i * step, step), step)
        left = sg[:, k]
        return (
            ga + jnp.dot(left, wg[k, :], preferred_element_type=F32),
            ua + jnp.dot(left, wu[k, :], preferred_element_type=F32),
        )

    zero = jnp.zeros((batch, hidden), F32)
    ga, ua = lax.fori_loop(0, width // step, project, (zero, zero))
    gu[0] = ga
    gu[1] = ua
    copies = []
    for d in range(1, nt):
        peer = lax.rem(tp + d, nt)
        copies.append(send(gu, gur.at[d - 1], t_s.at[1, d - 1], t_r.at[1, d - 1], tp=peer))
        copies.append(send(sqb, sqr.at[d - 1], t_s.at[2, d - 1], t_r.at[2, d - 1], tp=peer))
    for copy in copies:
        copy.wait()
    gate, up, squares = gu[0], gu[1], sqb[...]
    for d in range(nt - 1):
        gate, up, squares = gate + gur[d, 0], up + gur[d, 1], squares + sqr[d]
    inv = lax.rsqrt(squares[:, :1] / width_all + norm_floor)
    gate, up = gate * inv, up * inv
    inner = (gate / (1.0 + jnp.exp(-gate)) * up).astype(BF16)

    others[2].wait()
    wh = width // 2
    if wh % 256 == 0:
        for i in range(2):
            for k in range(0, wh, 256):
                fp[i, :, k : k + 256] = jnp.dot(
                    inner, wd[:, i * wh + k : i * wh + k + 256], preferred_element_type=F32
                )
    else:
        y = jnp.dot(inner, wd[...], preferred_element_type=F32)
        fp[0] = y[:, :wh]
        fp[1] = y[:, wh:]

    hb = batch // 2
    mine = pl.ds(pl.multiple_of(c * hb, hb), hb)
    theirs = pl.ds(pl.multiple_of((1 - c) * hb, hb), hb)
    send(fp.at[:, theirs, :], f1, f_s.at[0], f_r.at[0], kv=core_peer).wait()
    fa[...] = fp[:, mine, :] + f1[...]
    send(fa.at[1 - x], f2, f_s.at[1], f_r.at[1], kv=x_peer).wait()
    summed = fa[x] + f2[...]
    fb[...] = summed
    f3[z] = summed
    copies = [
        send(fb, f3.at[z], fz_s.at[d - 1], fz_r.at[d - 1], kv=z_peer(d)) for d in range(1, nz)
    ]
    for copy in copies:
        copy.wait()
    summed = f3[0]
    for i in range(1, nz):
        summed = summed + f3[i]
    fin2[x, mine, :] = summed
    part = fin2.at[x, mine, :]
    send(part, part, f_s.at[2], f_r.at[2], kv=x_peer).wait()
    part = fin2.at[:, mine, :]
    send(part, part, f_s.at[3], f_r.at[3], kv=core_peer).wait()
    for i in range(2):
        out[:, i * wh : (i + 1) * wh] = (st[:, i * wh : (i + 1) * wh] + fin2[i]).astype(out.dtype)


def per_device(n, nt, queries, cache, lengths, w_ov, resid, gain, w_gate, w_up, w_down):
    rows = cache.shape[1]
    first_row = lax.axis_index("kv") * rows
    place = first_row + lax.iota(jnp.int32, rows)
    live = (place[None, :] < lengths[:, None])[:, None, :]
    scores = jnp.einsum("bhc,brc->bhr", queries, cache, preferred_element_type=F32) * softmax_scale
    scores = jnp.where(live, scores, masked_score)
    peak = jnp.max(scores, axis=2)
    weights = jnp.where(live, jnp.exp(scores - peak[:, :, None]), 0.0)
    total = jnp.sum(weights, axis=2)
    mixed = jnp.einsum(
        "bhr,brc->hbc", weights.astype(BF16), cache[:, :, :LAT], preferred_element_type=F32
    )
    stats = jnp.stack([peak, total])

    batch, heads = peak.shape
    chunks = max(1, heads // 16)
    hc = heads // chunks
    nz = n // 4
    quarter = hc // 4
    piece_rows = quarter * batch // nz
    lat = LAT
    cols = w_ov.shape[2]
    width, hidden = w_gate.shape
    wh, hb = width // 2, batch // 2
    slots = min(3, chunks)
    if piece_rows % batch == 0:
        r3 = (chunks, nz - 1, piece_rows // batch, batch, lat)
    else:
        r3 = (chunks, nz - 1, piece_rows, lat)
    vm = pltpu.VMEM
    dma = pltpu.SemaphoreType.DMA
    scratch = [
        vm((n - 1, 2, batch, heads), F32),
        vm((heads, batch, lat), F32),
        vm((chunks, hc // 2, batch, lat), F32),
        vm((chunks, quarter, batch, lat), F32),
        vm(r3, F32),
        vm((heads, batch, lat), F32),
        vm((slots, hc, lat, cols), BF16),
        vm((width, hidden), BF16),
        vm((width, hidden), BF16),
        vm((hidden, width), BF16),
        vm((batch, cols), F32),
        vm((nt - 1, batch, cols), F32),
        vm((batch, cols), F32),
        vm((n // nt, batch, cols), F32),
        vm((batch, width), F32),
        vm((batch, width), BF16),
        vm((2, batch, hidden), F32),
        vm((nt - 1, 2, batch, hidden), F32),
        vm((batch, 128), F32),
        vm((nt - 1, batch, 128), F32),
        vm((2, batch, wh), F32),
        vm((2, hb, wh), F32),
        vm((2, hb, wh), F32),
        vm((hb, wh), F32),
        vm((hb, wh), F32),
        vm((nz, hb, wh), F32),
        vm((2, batch, wh), F32),
        dma((chunks + 3,)),
        dma((n - 1,)), dma((n - 1,)),
        dma((chunks, 4)), dma((chunks, 4)),
        dma((chunks, 2, nz - 1)), dma((chunks, 2, nz - 1)),
        dma((3, nt - 1)), dma((3, nt - 1)),
        dma((n - 1,)), dma((n // nt,)),
        dma((4,)), dma((4,)),
        dma((nz - 1,)), dma((nz - 1,)),
    ]
    in_vmem = pl.BlockSpec(memory_space=pltpu.VMEM)
    in_hbm = pl.BlockSpec(memory_space=pl.ANY)
    return pl.pallas_call(
        functools.partial(layer_kernel, n, nt, chunks, width * nt),
        out_shape=jax.ShapeDtypeStruct((batch, width), BF16),
        in_specs=[in_vmem] * 4 + [in_hbm] * 4,
        out_specs=in_vmem,
        scratch_shapes=scratch,
        compiler_params=pltpu.CompilerParams(
            collective_id=0, has_side_effects=True, vmem_limit_bytes=63 * 1024 * 1024
        ),
    )(stats, mixed, resid, gain.reshape(1, width), w_ov, w_gate, w_up, w_down)


def solution(mesh):
    in_specs = (
        P(None, "tp", None),
        P(None, "kv", None),
        P(),
        P("tp", None, "kv"),
        P(None, "tp"),
        P("tp"),
        P("tp", "kv"),
        P("tp", "kv"),
        P("kv", "tp"),
    )
    return jax.shard_map(
        functools.partial(per_device, mesh.shape["kv"], mesh.shape["tp"]),
        mesh=mesh,
        in_specs=in_specs,
        out_specs=P(None, "tp"),
        check_vma=False,
    )
```

```python
import functools

import jax
import jax.numpy as jnp
from jax import lax
from jax.experimental import pallas as pl
from jax.experimental.pallas import tpu as pltpu
from jax.sharding import PartitionSpec as P

LAT = 512
MESH = pl.DeviceIdType.MESH
F32 = jnp.float32
BF16 = jnp.bfloat16

softmax_scale = 192.0 ** (-0.5)
masked_score = -1e30
norm_floor = 0.05


def layer_kernel(
    n, nt, chunks, width_all,
    lens, q_hbm, cache_hbm, resid, gain, wov_hbm, wg_hbm, wu_hbm, wd_hbm,
    out,
    q, kt, wts, mixed, cols_ab, stats, qsem, ksem, sx, buf, r1, r2, r3, fin, wov, wg, wu, wd, pa, pr, pb, gath, st, sg, gu, gur, sqb, sqr,
    fp, f1, fa, f2, fb, f3, fin2,
    wsem, sx_s, sx_r, c_s, c_r, z_s, z_r, t_s, t_r, b_s, b_r, f_s, f_r, fz_s, fz_r,
):
    batch, heads, _ = q.shape
    lat = buf.shape[2]
    rows_kv = kt.shape[2]
    nz = n // 4
    hc = heads // chunks
    half, quarter = hc // 2, hc // 4
    rows = quarter * batch // nz
    slots = wov.shape[0]
    me, tp = lax.axis_index("kv"), lax.axis_index("tp")
    c, x, z = lax.rem(me, 2), lax.rem(me // 2, 2), me // 4
    core_peer, x_peer = me + 1 - 2 * c, me + 2 - 4 * x

    def z_peer(d):
        return lax.rem(z + d, nz) * 4 + x * 2 + c

    def send(src, dst, s, r, **where):
        copy = pltpu.make_async_remote_copy(
            src_ref=src, dst_ref=dst, send_sem=s, recv_sem=r, device_id=where, device_id_type=MESH
        )
        copy.start()
        return copy

    fetch = [pltpu.make_async_copy(q_hbm, q, qsem)]
    fetch += [pltpu.make_async_copy(cache_hbm.at[b], kt.at[b], ksem.at[b]) for b in range(batch)]
    for copy in fetch:
        copy.start()

    barrier = pltpu.get_barrier_semaphore()
    for d in range(1, n):
        pl.semaphore_signal(barrier, inc=1, device_id={"kv": lax.rem(me + d, n)}, device_id_type=MESH)
    for d in range(1, nt):
        pl.semaphore_signal(barrier, inc=1, device_id={"tp": lax.rem(tp + d, nt)}, device_id_type=MESH)
    place = me * rows_kv + lax.broadcasted_iota(jnp.int32, (heads, rows_kv), 1)
    fetch[0].wait()
    for b in range(batch):
        fetch[1 + b].wait()
        live = place < lens[b]
        scores = jnp.dot(q[b], kt[b], preferred_element_type=F32) * softmax_scale
        scores = jnp.where(live, scores, masked_score)
        high = jnp.max(scores, axis=1, keepdims=True)
        soft = jnp.where(live, jnp.exp(scores - high), 0.0)
        wts[b] = soft.astype(BF16)
        cols_ab[:, b : b + 1] = high
        cols_ab[:, batch + b : batch + b + 1] = jnp.sum(soft, axis=1, keepdims=True)
    turned = cols_ab[...].T
    stats[0] = turned[:batch]
    stats[1] = turned[batch : 2 * batch]

    loads = {}

    def load_ov(ch):
        loads[ch] = pltpu.make_async_copy(
            wov_hbm.at[pl.ds(ch * hc, hc)], wov.at[ch % slots], wsem.at[ch]
        )
        loads[ch].start()

    for ch in range(slots):
        load_ov(ch)
    others = []
    for i, (a, b) in enumerate(((wg_hbm, wg), (wu_hbm, wu), (wd_hbm, wd))):
        copy = pltpu.make_async_copy(a, b, wsem.at[chunks + i])
        copy.start()
        others.append(copy)

    pl.semaphore_wait(barrier, n - 1 + nt - 1)

    copies = [
        send(stats, sx.at[d - 1], sx_s.at[d - 1], sx_r.at[d - 1], kv=lax.rem(me + d, n))
        for d in range(1, n)
    ]
    for b in range(batch):
        whole_row = lax.dot_general(
            wts[b], kt[b, :lat, :], (((1,), (1,)), ((), ())), preferred_element_type=F32
        )
        for k in range(lat // 128):
            mixed[k, pl.ds(b * heads, heads), :] = whole_row[:, k * 128 : (k + 1) * 128]
    for copy in copies:
        copy.wait()
    peak, total = stats[0], stats[1]
    top = peak
    for d in range(n - 1):
        top = jnp.maximum(top, sx[d, 0])
    factor = jnp.exp(peak - top)
    whole = total * factor
    for d in range(n - 1):
        whole = whole + sx[d, 1] * jnp.exp(sx[d, 0] - top)
    factor = factor / whole

    def piece(ref, h0, zz):
        if rows % batch == 0:
            return ref.at[pl.ds(h0 + zz * (rows // batch), rows // batch)]
        return ref.at[h0 + zz * rows // batch, pl.ds(pl.multiple_of(lax.rem(zz * rows, batch), rows), rows)]

    flight = {}
    acc = [jnp.zeros((batch, pa.shape[1]), F32)]

    def stage(ch, s):
        b = ch * hc
        h0 = b + c * half
        q0 = h0 + x * quarter
        for copy in flight.pop(ch, ()):
            copy.wait()
        if s == 0:
            for i in range(hc):
                scale = factor[:, b + i : b + i + 1]
                for k in range(lat // 128):
                    buf[b + i, :, k * 128 : (k + 1) * 128] = mixed[k, pl.ds(b + i, batch, stride=heads), :] * scale
            flight[ch] = [
                send(buf.at[pl.ds(b + (1 - c) * half, half)], r1.at[ch], c_s.at[ch, 0], c_r.at[ch, 0], kv=core_peer)
            ]
        elif s == 1:
            for i in range(half):
                buf[h0 + i] = buf[h0 + i] + r1[ch, i]
            flight[ch] = [
                send(buf.at[pl.ds(h0 + (1 - x) * quarter, quarter)], r2.at[ch], c_s.at[ch, 1], c_r.at[ch, 1], kv=x_peer)
            ]
        elif s == 2:
            for i in range(quarter):
                buf[q0 + i] = buf[q0 + i] + r2[ch, i]
            flight[ch] = [
                send(piece(buf, q0, lax.rem(z + d, nz)), r3.at[ch, d - 1], z_s.at[ch, 0, d - 1], z_r.at[ch, 0, d - 1], kv=z_peer(d))
                for d in range(1, nz)
            ]
        elif s == 3:
            own = piece(buf, q0, z)[...]
            for d in range(nz - 1):
                own = own + r3[ch, d].reshape(own.shape)
            mine = piece(fin, q0, z)
            mine[...] = own
            flight[ch] = [
                send(mine, mine, z_s.at[ch, 1, d - 1], z_r.at[ch, 1, d - 1], kv=z_peer(d)) for d in range(1, nz)
            ]
        elif s == 4:
            part = fin.at[pl.ds(q0, quarter)]
            flight[ch] = [send(part, part, c_s.at[ch, 2], c_r.at[ch, 2], kv=x_peer)]
        elif s == 5:
            part = fin.at[pl.ds(h0, half)]
            flight[ch] = [send(part, part, c_s.at[ch, 3], c_r.at[ch, 3], kv=core_peer)]
        else:
            loads[ch].wait()

            def body(i, a):
                return a + lax.dot_general(
                    fin[b + i].astype(BF16), wov[ch % slots, i], (((1,), (1,)), ((), ())),
                    preferred_element_type=F32,
                )

            acc[0] = lax.fori_loop(0, hc, body, acc[0])
            if ch + slots < chunks:
                load_ov(ch + slots)

    for t in range(chunks + 6):
        turn = [(ch, t - ch) for ch in range(chunks) if 0 <= t - ch <= 6]
        for ch, s in sorted(turn, key=lambda e: e[1] == 6):
            stage(ch, s)

    pa[...] = acc[0]
    copies = [
        send(pa, pr.at[d - 1], t_s.at[0, d - 1], t_r.at[0, d - 1], tp=lax.rem(tp + d, nt)) for d in range(1, nt)
    ]
    own = pa[...]
    for copy in copies:
        copy.wait()
    for d in range(nt - 1):
        own = own + pr[d]
    pb[...] = own
    per = n // nt
    slot = lax.rem(me, per)
    owner = me // per == tp

    def spread(d):
        return pltpu.make_async_remote_copy(
            src_ref=pb, dst_ref=gath.at[slot], send_sem=b_s.at[d - 1], recv_sem=b_r.at[slot],
            device_id={"kv": lax.rem(me + d, n)}, device_id_type=MESH,
        )

    @pl.when(owner)
    def _():
        for d in range(1, n):
            spread(d).start()
        gath[slot] = pb[...]
        for d in range(1, n):
            spread(d).wait_send()

    for j in range(per):
        @pl.when(tp * per + j != me)
        def _():
            pltpu.make_async_remote_copy(
                src_ref=pb, dst_ref=gath.at[j], send_sem=b_s.at[0], recv_sem=b_r.at[j],
                device_id={"kv": me}, device_id_type=MESH,
            ).wait_recv()

    cols = pb.shape[1]
    for j in range(per):
        st[:, j * cols : (j + 1) * cols] = gath[j]
    width, hidden = wg.shape
    state = st[...] + resid[...].astype(F32)
    st[...] = state
    sqb[...] = jnp.broadcast_to(jnp.sum(state * state, axis=1, keepdims=True), sqb.shape)
    sg[...] = (state * gain[...].reshape(1, width)).astype(BF16)

    step = 512 if width % 512 == 0 else 128
    others[0].wait()
    others[1].wait()

    def project(i, carry):
        ga, ua = carry
        k = pl.ds(pl.multiple_of(i * step, step), step)
        left = sg[:, k]
        return (
            ga + jnp.dot(left, wg[k, :], preferred_element_type=F32),
            ua + jnp.dot(left, wu[k, :], preferred_element_type=F32),
        )

    zero = jnp.zeros((batch, hidden), F32)
    ga, ua = lax.fori_loop(0, width // step, project, (zero, zero))
    gu[0] = ga
    gu[1] = ua
    copies = []
    for d in range(1, nt):
        peer = lax.rem(tp + d, nt)
        copies.append(send(gu, gur.at[d - 1], t_s.at[1, d - 1], t_r.at[1, d - 1], tp=peer))
        copies.append(send(sqb, sqr.at[d - 1], t_s.at[2, d - 1], t_r.at[2, d - 1], tp=peer))
    for copy in copies:
        copy.wait()
    gate, up, squares = gu[0], gu[1], sqb[...]
    for d in range(nt - 1):
        gate, up, squares = gate + gur[d, 0], up + gur[d, 1], squares + sqr[d]
    inv = lax.rsqrt(squares[:, :1] / width_all + norm_floor)
    gate, up = gate * inv, up * inv
    inner = (gate / (1.0 + jnp.exp(-gate)) * up).astype(BF16)

    others[2].wait()
    wh = width // 2
    if wh % 256 == 0:
        for i in range(2):
            for k in range(0, wh, 256):
                fp[i, :, k : k + 256] = jnp.dot(
                    inner, wd[:, i * wh + k : i * wh + k + 256], preferred_element_type=F32
                )
    else:
        y = jnp.dot(inner, wd[...], preferred_element_type=F32)
        fp[0] = y[:, :wh]
        fp[1] = y[:, wh:]

    hb = batch // 2
    mine = pl.ds(pl.multiple_of(c * hb, hb), hb)
    theirs = pl.ds(pl.multiple_of((1 - c) * hb, hb), hb)
    send(fp.at[:, theirs, :], f1, f_s.at[0], f_r.at[0], kv=core_peer).wait()
    fa[...] = fp[:, mine, :] + f1[...]
    send(fa.at[1 - x], f2, f_s.at[1], f_r.at[1], kv=x_peer).wait()
    summed = fa[x] + f2[...]
    fb[...] = summed
    f3[z] = summed
    copies = [
        send(fb, f3.at[z], fz_s.at[d - 1], fz_r.at[d - 1], kv=z_peer(d)) for d in range(1, nz)
    ]
    for copy in copies:
        copy.wait()
    summed = f3[0]
    for i in range(1, nz):
        summed = summed + f3[i]
    fin2[x, mine, :] = summed
    part = fin2.at[x, mine, :]
    send(part, part, f_s.at[2], f_r.at[2], kv=x_peer).wait()
    part = fin2.at[:, mine, :]
    send(part, part, f_s.at[3], f_r.at[3], kv=core_peer).wait()
    for i in range(2):
        out[:, i * wh : (i + 1) * wh] = (st[:, i * wh : (i + 1) * wh] + fin2[i]).astype(out.dtype)


def per_device(n, nt, queries, cache, lengths, w_ov, resid, gain, w_gate, w_up, w_down):
    batch, heads, entries = queries.shape
    rows_kv = cache.shape[1]
    chunks = max(1, heads // 16)
    hc = heads // chunks
    nz = n // 4
    quarter = hc // 4
    piece_rows = quarter * batch // nz
    lat = LAT
    cols = w_ov.shape[2]
    width, hidden = w_gate.shape
    wh, hb = width // 2, batch // 2
    slots = min(3, chunks)
    if piece_rows % batch == 0:
        r3 = (chunks, nz - 1, piece_rows // batch, batch, lat)
    else:
        r3 = (chunks, nz - 1, piece_rows, lat)
    vm = pltpu.VMEM
    dma = pltpu.SemaphoreType.DMA
    scratch = [
        vm((batch, heads, entries), BF16),
        vm((batch, entries, rows_kv), BF16),
        vm((batch, heads, rows_kv), BF16),
        vm((lat // 128, batch * heads, 128), F32),
        vm((heads, 128), F32),
        vm((2, batch, heads), F32),
        dma(()), dma((batch,)),
        vm((n - 1, 2, batch, heads), F32),
        vm((heads, batch, lat), F32),
        vm((chunks, hc // 2, batch, lat), F32),
        vm((chunks, quarter, batch, lat), F32),
        vm(r3, F32),
        vm((heads, batch, lat), F32),
        vm((slots, hc, cols, lat), BF16),
        vm((width, hidden), BF16),
        vm((width, hidden), BF16),
        vm((hidden, width), BF16),
        vm((batch, cols), F32),
        vm((nt - 1, batch, cols), F32),
        vm((batch, cols), F32),
        vm((n // nt, batch, cols), F32),
        vm((batch, width), F32),
        vm((batch, width), BF16),
        vm((2, batch, hidden), F32),
        vm((nt - 1, 2, batch, hidden), F32),
        vm((batch, 128), F32),
        vm((nt - 1, batch, 128), F32),
        vm((2, batch, wh), F32),
        vm((2, hb, wh), F32),
        vm((2, hb, wh), F32),
        vm((hb, wh), F32),
        vm((hb, wh), F32),
        vm((nz, hb, wh), F32),
        vm((2, batch, wh), F32),
        dma((chunks + 3,)),
        dma((n - 1,)), dma((n - 1,)),
        dma((chunks, 4)), dma((chunks, 4)),
        dma((chunks, 2, nz - 1)), dma((chunks, 2, nz - 1)),
        dma((3, nt - 1)), dma((3, nt - 1)),
        dma((n - 1,)), dma((n // nt,)),
        dma((4,)), dma((4,)),
        dma((nz - 1,)), dma((nz - 1,)),
    ]
    in_vmem = pl.BlockSpec(memory_space=pltpu.VMEM)
    in_hbm = pl.BlockSpec(memory_space=pl.ANY)
    return pl.pallas_call(
        functools.partial(layer_kernel, n, nt, chunks, width * nt),
        out_shape=jax.ShapeDtypeStruct((batch, width), BF16),
        in_specs=[pl.BlockSpec(memory_space=pltpu.SMEM)] + [in_hbm] * 2 + [in_vmem] * 2 + [in_hbm] * 4,
        out_specs=in_vmem,
        scratch_shapes=scratch,
        compiler_params=pltpu.CompilerParams(
            collective_id=0, has_side_effects=True, vmem_limit_bytes=63 * 1024 * 1024
        ),
    )(lengths, queries, jnp.swapaxes(cache, 1, 2), resid, gain, jnp.swapaxes(w_ov, 1, 2), w_gate, w_up, w_down)


def solution(mesh):
    in_specs = (
        P(None, "tp", None),
        P(None, "kv", None),
        P(),
        P("tp", None, "kv"),
        P(None, "tp"),
        P("tp"),
        P("tp", "kv"),
        P("tp", "kv"),
        P("kv", "tp"),
    )
    return jax.shard_map(
        functools.partial(per_device, mesh.shape["kv"], mesh.shape["tp"]),
        mesh=mesh,
        in_specs=in_specs,
        out_specs=P(None, "tp"),
        check_vma=False,
    )
```
